1024 devices in a mesh: dp: 32 (over y, z_hi, core), tensor: 32 (over x, z_lo).
Axes of the slice: x: 4, y: 4, z: 32 (z_hi: 4, z_lo: 8; z = z_hi * 8 + z_lo), core: 2. Of those that a mesh axis runs over, the one named last changes fastest.
Arguments:
- attn_input: bfloat16 [4096, 8192], P('dp'), may hold values from -6 to 6
- residual: bfloat16 [4096, 8192], P('dp'), may hold values from -3 to 3
- query_weight: bfloat16 [8192, 8192], P('dp', 'tensor'), may hold values from -0.0625 to 0.0625
- query_bias: bfloat16 [8192], P('tensor'), may hold values from -3 to 3
- output_weight: bfloat16 [8192, 8192], P('tensor', 'dp'), may hold values from -0.0625 to 0.0625
- cached_keys: bfloat16 [32, 32, 1024, 128], P('dp', 'tensor'), may hold values from -305 to 305, as said below
- cached_values: bfloat16 [32, 32, 1024, 128], P('dp', 'tensor'), may hold values from -12 to 12, as said below
- norm_gain: bfloat16 [8192], replicated, may hold values from 0.5 to 1.5
Outputs:
- hidden_out: bfloat16 [4096, 8192], P(('dp', 'tensor'))
- normed_out: bfloat16 [4096, 8192], P('dp')
The draws below stay inside these ranges and needn't reach their ends.
Inputs may be any that keep to these rules, and one draw needn't show every extreme that they name: `cached_keys`: groups g and g2 with g // 4 == g2 // 4 carry equal keys. `cached_values`: groups g and g2 with g // 4 == g2 // 4 carry equal values.
All inputs are finite; a program needn't handle non-finite values.
Results may differ from the reference program's by a relative error of at most 0.025.
Values may be sent and summed in bfloat16 or wider, within the bound.
A program may use at most 64 MiB of HBM per device.

```python
import jax
import jax.numpy as jnp
from jax import lax

D = 8192
HD = 128
KVH = 8
QH_DEV = 2
TOK = 128
CTX = 1024
HEADS = 64
N_DP = 32
N_TENSOR = 32


def draw_cached_keys(key, part):
    base_key = jax.random.fold_in(key, 11)
    full_shape = (N_DP, KVH, CTX, HD)
    drawn = 2.0 * jax.random.truncated_normal(base_key, -6.0, 6.0, full_shape, jnp.float32)
    packed = drawn.astype(jnp.bfloat16)
    return jnp.repeat(packed, N_TENSOR // KVH, axis=1)


def draw_cached_values(key, part):
    base_key = jax.random.fold_in(key, 37)
    full_shape = (N_DP, KVH, CTX, HD)
    drawn = 2.0 * jax.random.truncated_normal(base_key, -6.0, 6.0, full_shape, jnp.float32)
    packed = drawn.astype(jnp.bfloat16)
    return jnp.repeat(packed, N_TENSOR // KVH, axis=1)


def levels(key, shape, cuts, least, largest):
    loudness, own = 1.0, jax.random.fold_in(key, 6)
    for dim, shards_of in cuts:
        steps = jnp.exp(jax.random.uniform(jax.random.fold_in(own, dim), (shards_of,), jnp.float32, least / len(cuts), largest / len(cuts)))
        loudness = loudness * jnp.repeat(steps, shape[dim] // shards_of).reshape([-1 if axis == dim else 1 for axis in range(len(shape))])
    return loudness


def noise(rng, shape, scale, limit, pieces=(), kind=jnp.bfloat16):
    values = jax.random.normal(rng, shape, jnp.float32) * scale
    if len(pieces) > 0:
        values = levels(rng, shape, pieces, -0.22, 0.18) * values
    return jnp.clip(values, min=-limit, max=limit).astype(kind)


def setup_inputs(seed: int = 0) -> dict:
    arg_keys = jax.random.split(jax.random.key(seed), 9)
    return {
        "attn_input": noise(arg_keys[0], (N_DP * TOK, D), 1.0, 6.0, ((0, 32),)),
        "residual": noise(arg_keys[1], (N_DP * TOK, D), 0.5, 3.0, ((0, 32),)),
        "query_weight": noise(arg_keys[2], (D, HEADS * HD), D ** -0.5, 0.0625, ((0, 32), (1, 32))),
        "query_bias": noise(arg_keys[3], (HEADS * HD,), 0.5, 3.0, ((0, 32),)),
        "output_weight": noise(arg_keys[4], (HEADS * HD, D), (HEADS * HD) ** -0.5, 0.0625, ((0, 32), (1, 32))),
        "cached_keys": draw_cached_keys(jax.random.fold_in(arg_keys[8], 71), 0),
        "cached_values": draw_cached_values(jax.random.fold_in(arg_keys[8], 71), 0),
        "norm_gain": jnp.clip(1.0 + 0.1 * jax.random.normal(arg_keys[7], (D,), jnp.float32), 0.5, 1.5).astype(jnp.bfloat16),
    }


rope_theta = 1000000.0
norm_eps = 1e-06

def rotate(projected, first_pos):
    head_dim = projected.shape[-1]
    half_dim = head_dim // 2
    inv_freq = jnp.power(jnp.float32(rope_theta), -2.0 * jnp.arange(half_dim, dtype=jnp.float32) / head_dim)
    positions = first_pos + jnp.arange(projected.shape[0], dtype=jnp.float32)
    angles = positions[:, None] * inv_freq[None, :]
    cosine = jnp.cos(angles)[:, None, :]
    sine = jnp.sin(angles)[:, None, :]
    first_half = projected[..., :half_dim]
    second_half = projected[..., half_dim:]
    return jnp.concatenate([first_half * cosine - second_half * sine, second_half * cosine + first_half * sine], axis=-1)

def attend(queries, group_keys, group_values):
    count_q = queries.shape[0]
    groups = group_keys.shape[0]
    count_k = group_keys.shape[1]
    grouped = queries.reshape(count_q, groups, queries.shape[1] // groups, queries.shape[2]).astype(jnp.float32)
    scores = jnp.einsum('tgqd,gkd->gqtk', grouped, group_keys.astype(jnp.float32)) * (1.0 / queries.shape[-1] ** 0.5)
    visible = jnp.arange(count_k)[None, :] <= (count_k - count_q + jnp.arange(count_q))[:, None]
    scores = jnp.where(visible[None, None], scores, jnp.float32(-1e+30))
    highest = lax.optimization_barrier(jnp.max(scores, axis=-1, keepdims=True))
    expo = jnp.exp(scores - highest)
    soft = (expo / lax.optimization_barrier(jnp.sum(expo, axis=-1, keepdims=True))).astype(jnp.bfloat16)
    mixed = jnp.einsum('gqtk,gkd->tgqd', soft.astype(jnp.float32), group_values.astype(jnp.float32))
    return mixed.reshape(queries.shape).astype(jnp.bfloat16)

def reference(attn_input, residual, query_weight, query_bias, output_weight, cached_keys, cached_values, norm_gain):
    groups = HEADS // QH_DEV
    weight_blocks = output_weight.reshape(groups, QH_DEV * HD, D)

    def one_sequence(group_items):
        inputs, resid_rows, group_keys, group_values = group_items
        projected = jnp.dot(inputs, query_weight, preferred_element_type=jnp.float32) + query_bias.astype(jnp.float32)
        queries = rotate(projected.reshape(TOK, HEADS, HD), float(CTX - TOK)).astype(jnp.bfloat16)
        mixed = attend(queries, group_keys, group_values).reshape(TOK, groups, QH_DEV * HD).transpose(1, 0, 2)

        def add_group(running, operands):
            group_part = jnp.dot(operands[0], operands[1], preferred_element_type=jnp.float32).astype(jnp.bfloat16)
            group_part = lax.optimization_barrier(group_part)
            return (running + group_part.astype(jnp.float32), None)
        summed, unused = lax.scan(add_group, jnp.zeros((TOK, D), jnp.float32), (mixed, weight_blocks))
        total = resid_rows.astype(jnp.float32) + summed
        mean_square = lax.optimization_barrier(jnp.mean(total * total, axis=-1, keepdims=True))
        normed = total * lax.rsqrt(mean_square + norm_eps) * norm_gain.astype(jnp.float32)
        return (total.astype(jnp.bfloat16), normed.astype(jnp.bfloat16))
    hidden, normed = lax.map(one_sequence, (attn_input.reshape(N_DP, TOK, D), residual.reshape(N_DP, TOK, D), cached_keys, cached_values))
    return (hidden.reshape(N_DP * TOK, D), normed.reshape(N_DP * TOK, D))
```

```python
import jax
import jax.numpy as jnp
import numpy as np
from jax import lax
from jax.experimental import pallas as pl
from jax.experimental.pallas import tpu as pltpu
from jax.sharding import PartitionSpec as P

rope_theta = 1000000.0
norm_eps = 1e-06

NY, NH, NC = 4, 4, 2
NX, NZ = 4, 8
OWN, PREV, NEXT, FAR = 0, 1, 2, 3
STEP = (0, 3, 1, 2)
F32, BF16 = jnp.float32, jnp.bfloat16


def block_kernel(
    x_hbm, wq_hbm, wo_hbm, k_hbm, v_hbm, bias_ref, cos_ref, sin_ref, res_ref, gain_ref,
    hid_ref, norm_hbm,
    w, xv, kv, vv, q, mixed, part, x1, x2, xsum, zrecv, tot, nbuf,
    loc, out_sem, zs, zr, ys, yr, ds, dr, p1s, p1r, p2s, p2r, rs, rr, gzs, gzr, gxs, gxr,
):
    dp = lax.axis_index("dp")
    ti = lax.axis_index("tensor")
    y, h, c = dp // (NH * NC), (dp // NC) % NH, dp % NC
    x, zl = ti // NZ, ti % NZ

    def piece(yy, hh, cc):
        return yy * (NH * NC) + hh * NC + cc

    def ring(base, slot):
        return (base + STEP[slot]) % 4

    def dev(d):
        return {"dp": d}

    def ten(t):
        return {"tensor": t}

    h_up, h_dn = dev(piece(y, ring(h, NEXT), c)), dev(piece(y, ring(h, PREV), c))
    y_up, y_dn = dev(piece(ring(y, NEXT), h, c)), dev(piece(ring(y, PREV), h, c))
    sib = dev(piece(y, h, 1 - c))
    x_up, x_dn = ten(ring(x, NEXT) * NZ + zl), ten(ring(x, PREV) * NZ + zl)

    locals_ = [
        pltpu.make_async_copy(wq_hbm, w.at[0, dp], loc.at[0]),
        pltpu.make_async_copy(wo_hbm, w.at[1, dp], loc.at[1]),
        pltpu.make_async_copy(x_hbm, xv, loc.at[2]),
        pltpu.make_async_copy(k_hbm, kv, loc.at[3]),
        pltpu.make_async_copy(v_hbm, vv, loc.at[4]),
    ]
    for copy in locals_:
        copy.start()

    barrier = pltpu.get_barrier_semaphore()
    partners = [h_up, h_dn, y_up, y_dn, sib, x_up, x_dn]
    partners += [ten(x * NZ + (zl + o) % NZ) for o in range(1, NZ)]
    for partner in partners:
        pl.semaphore_signal(
            barrier, inc=1, device_id=partner, device_id_type=pl.DeviceIdType.MESH
        )
    pl.semaphore_wait(barrier, len(partners))
    locals_[0].wait()
    locals_[1].wait()

    sent = []

    def remote(src, dst, send_sem, recv_sem, target):
        return pltpu.make_async_remote_copy(
            src_ref=src, dst_ref=dst, send_sem=send_sem, recv_sem=recv_sem,
            device_id=target, device_id_type=pl.DeviceIdType.MESH,
        )

    def send(src, dst, send_sem, recv_sem, target):
        copy = remote(src, dst, send_sem, recv_sem, target)
        copy.start()
        sent.append(copy)

    def landed(dst, send_sem, recv_sem):
        remote(dst, dst, send_sem, recv_sem, sib).wait_recv()

    def w_at(m, ky, kh, half):
        return w.at[m, piece(ring(y, ky), ring(h, kh), c), half]

    def push(ref, s, r, i, target):
        send(ref, ref, s.at[i], r.at[i], target)

    def z_start(m):
        s, r = zs.at[m], zr.at[m]
        push(w_at(m, OWN, OWN, 0), s, r, 0, h_up)
        push(w_at(m, OWN, OWN, 1), s, r, 3, h_dn)
        push(w_at(m, OWN, OWN, 1), s, r, 1, h_up)
        push(w_at(m, OWN, OWN, 0), s, r, 4, h_dn)

    def y_start(m, k, half):
        s, r = ys.at[m, k], yr.at[m, k]
        if half == 0:
            push(w_at(m, OWN, k, 0), s, r, 0, y_up)
            push(w_at(m, OWN, k, 0), s, r, 4, y_dn)
        else:
            push(w_at(m, OWN, k, 1), s, r, 3, y_dn)
            push(w_at(m, OWN, k, 1), s, r, 1, y_up)

    def d_start(m, k, ky):
        ref = w.at[m, piece(ring(y, ky), ring(h, k), c)]
        push(ref, ds.at[m, k], dr.at[m, k], ky, sib)

    def z_first(m):
        s, r = zs.at[m], zr.at[m]
        landed(w_at(m, OWN, PREV, 0), s.at[0], r.at[0])
        push(w_at(m, OWN, PREV, 0), s, r, 2, h_up)
        landed(w_at(m, OWN, NEXT, 1), s.at[3], r.at[3])
        push(w_at(m, OWN, NEXT, 1), s, r, 5, h_dn)
        y_start(m, PREV, 0)
        y_start(m, NEXT, 1)

    def z_second(m):
        s, r = zs.at[m], zr.at[m]
        landed(w_at(m, OWN, PREV, 1), s.at[1], r.at[1])
        y_start(m, PREV, 1)
        d_start(m, PREV, OWN)
        landed(w_at(m, OWN, NEXT, 0), s.at[4], r.at[4])
        y_start(m, NEXT, 0)
        d_start(m, NEXT, OWN)

    def z_third(m):
        s, r = zs.at[m], zr.at[m]
        landed(w_at(m, OWN, FAR, 0), s.at[2], r.at[2])
        y_start(m, FAR, 0)
        landed(w_at(m, OWN, FAR, 1), s.at[5], r.at[5])
        y_start(m, FAR, 1)
        d_start(m, FAR, OWN)

    def y_first(m, k):
        s, r = ys.at[m, k], yr.at[m, k]
        landed(w_at(m, PREV, k, 0), s.at[0], r.at[0])
        push(w_at(m, PREV, k, 0), s, r, 2, y_up)
        landed(w_at(m, NEXT, k, 1), s.at[3], r.at[3])
        push(w_at(m, NEXT, k, 1), s, r, 5, y_dn)

    def y_second(m, k):
        s, r = ys.at[m, k], yr.at[m, k]
        landed(w_at(m, PREV, k, 1), s.at[1], r.at[1])
        d_start(m, k, PREV)
        landed(w_at(m, NEXT, k, 0), s.at[4], r.at[4])
        d_start(m, k, NEXT)

    def y_third(m, k):
        s, r = ys.at[m, k], yr.at[m, k]
        landed(w_at(m, FAR, k, 0), s.at[2], r.at[2])
        landed(w_at(m, FAR, k, 1), s.at[5], r.at[5])
        d_start(m, k, FAR)

    def d_landed(m, k):
        for ky in range(4):
            ref = w.at[m, piece(ring(y, ky), ring(h, k), 1 - c)]
            landed(ref, ds.at[m, k, ky], dr.at[m, k, ky])

    def project(k):
        d_landed(0, k)
        hk = ring(h, k)

        def one(j, carry):
            d = piece(j // NC, hk, j % NC)
            cols = xv[:, pl.ds(pl.multiple_of(d * 256, 256), 256)]
            weights = w[0, d].reshape(256, 256)
            q[...] += jnp.dot(cols, weights, preferred_element_type=F32)
            return carry

        lax.fori_loop(0, NY * NC, one, 0)

    def attend(head):
        cols = slice(head * 128, head * 128 + 128)
        proj = q[:, cols] + bias_ref[:, cols].astype(F32)
        turned = proj * cos_ref[...] + pltpu.roll(proj, 64, 1) * sin_ref[...]
        scores = lax.dot_general(
            turned.astype(BF16), kv[...], (((1,), (1,)), ((), ())), preferred_element_type=F32
        ) * (1.0 / 128**0.5)
        rows = lax.broadcasted_iota(jnp.int32, scores.shape, 0)
        keys = lax.broadcasted_iota(jnp.int32, scores.shape, 1)
        scores = jnp.where(keys <= rows + (scores.shape[1] - scores.shape[0]), scores, -1e30)
        expo = jnp.exp(scores - jnp.max(scores, axis=-1, keepdims=True))
        soft = (expo / jnp.sum(expo, axis=-1, keepdims=True)).astype(BF16)
        mixed[:, cols] = jnp.dot(soft, vv[...], preferred_element_type=F32).astype(BF16)

    def partials(k):
        d_landed(1, k)
        hk = ring(h, k)

        def one(j, carry):
            d = piece(j // NC, hk, j % NC)
            out = jnp.dot(mixed[...], w[1, d].reshape(256, 256), preferred_element_type=F32)
            cols = pl.ds(pl.multiple_of(j * 256, 256), 256)
            part[hk, :, :, cols] = out.astype(BF16).reshape(32, 4, 256)
            return carry

        lax.fori_loop(0, NY * NC, one, 0)

    def rows_of(k, slot, at, count):
        return part.at[ring(h, k), pl.ds(ring(x, slot) * NZ + at, count)]

    def sum_first(k):
        send(rows_of(k, FAR, 0, 4), x1.at[k, 0], p1s.at[k, 0], p1r.at[k, 0], x_up)
        send(rows_of(k, FAR, 4, 4), x1.at[k, 1], p1s.at[k, 1], p1r.at[k, 1], x_dn)
        send(rows_of(k, NEXT, 4, 4), x2.at[k, 0, 1], p2s.at[k, 0], p2r.at[k, 0], x_up)
        send(rows_of(k, PREV, 0, 4), x2.at[k, 1, 0], p2s.at[k, 1], p2r.at[k, 1], x_dn)

    def sum_second(k):
        landed(x1.at[k, 0], p1s.at[k, 0], p1r.at[k, 0])
        own = rows_of(k, NEXT, 0, 4)
        own[...] = (own[...].astype(F32) + x1[k, 0].astype(F32)).astype(BF16)
        send(own, x2.at[k, 0, 0], p2s.at[k, 2], p2r.at[k, 2], x_up)
        landed(x1.at[k, 1], p1s.at[k, 1], p1r.at[k, 1])
        own = rows_of(k, PREV, 4, 4)
        own[...] = (own[...].astype(F32) + x1[k, 1].astype(F32)).astype(BF16)
        send(own, x2.at[k, 1, 1], p2s.at[k, 3], p2r.at[k, 3], x_dn)

    def sum_third(k):
        landed(x2.at[k, 0, 1], p2s.at[k, 0], p2r.at[k, 0])
        landed(x2.at[k, 1, 0], p2s.at[k, 1], p2r.at[k, 1])
        landed(x2.at[k, 0, 0], p2s.at[k, 2], p2r.at[k, 2])
        landed(x2.at[k, 1, 1], p2s.at[k, 3], p2r.at[k, 3])
        for half in range(2):
            own = rows_of(k, OWN, half * 4, 4)[...].astype(F32)
            both = x2[k, 0, half].astype(F32) + x2[k, 1, half].astype(F32)
            xsum[k, half * 4 : half * 4 + 4] = (own + both).astype(BF16)
        for o in range(1, NZ):
            there = (zl + o) % NZ
            send(xsum.at[k, there], zrecv.at[k, o - 1], rs.at[k, o - 1], rr.at[k, o - 1],
                 ten(x * NZ + there))

    def gathered(k):
        acc = xsum[k, zl].astype(F32)
        for o in range(1, NZ):
            landed(zrecv.at[k, o - 1], rs.at[k, o - 1], rr.at[k, o - 1])
            acc = acc + zrecv[k, o - 1].astype(F32)
        hk = ring(h, k)
        for j in range(NY * NC):
            d = piece(j // NC, hk, j % NC)
            tot[:, pl.ds(pl.multiple_of(d * 256, 256), 256)] = acc[:, j * 256 : j * 256 + 256]

    q[...] = jnp.zeros_like(q)
    z_start(0)
    for m in range(2):
        y_start(m, OWN, 0)
        y_start(m, OWN, 1)
        d_start(m, OWN, OWN)
    for m in range(2):
        y_first(m, OWN)
        y_second(m, OWN)
        y_third(m, OWN)
    locals_[2].wait()
    project(OWN)
    z_first(0)
    z_start(1)
    z_second(0)
    y_first(0, PREV)
    y_first(0, NEXT)
    y_second(0, PREV)
    y_second(0, NEXT)
    y_third(0, PREV)
    y_third(0, NEXT)
    project(PREV)
    project(NEXT)
    z_third(0)
    y_first(0, FAR)
    y_second(0, FAR)
    y_third(0, FAR)
    project(FAR)
    locals_[3].wait()
    locals_[4].wait()
    attend(0)
    z_first(1)
    attend(1)
    partials(OWN)
    sum_first(OWN)
    z_second(1)
    y_first(1, PREV)
    y_first(1, NEXT)
    y_second(1, PREV)
    y_second(1, NEXT)
    sum_second(OWN)
    y_third(1, PREV)
    y_third(1, NEXT)
    partials(PREV)
    sum_first(PREV)
    sum_third(OWN)
    partials(NEXT)
    sum_first(NEXT)
    z_third(1)
    y_first(1, FAR)
    sum_second(PREV)
    sum_second(NEXT)
    y_second(1, FAR)
    y_third(1, FAR)
    sum_third(PREV)
    sum_third(NEXT)
    partials(FAR)
    sum_first(FAR)
    gathered(OWN)
    sum_second(FAR)
    sum_third(FAR)
    gathered(PREV)
    gathered(NEXT)
    gathered(FAR)

    total = tot[...] + res_ref[...].astype(F32)
    hid_ref[...] = total.astype(BF16)
    mean_square = jnp.mean(total * total, axis=-1, keepdims=True)
    normed = total * lax.rsqrt(mean_square + norm_eps) * gain_ref[...].astype(F32)
    nbuf[ti] = normed.astype(BF16)

    def n_at(kx, o):
        return nbuf.at[ring(x, kx) * NZ + (zl - o) % NZ]

    def gx_start(o):
        s, r = gxs.at[o], gxr.at[o]
        push(n_at(OWN, o), s, r, 0, x_up)
        push(n_at(OWN, o), s, r, 1, x_dn)

    def gx_next(o):
        s, r = gxs.at[o], gxr.at[o]
        landed(n_at(PREV, o), s.at[0], r.at[0])
        push(n_at(PREV, o).at[:, :4096], s, r, 2, x_up)
        landed(n_at(NEXT, o), s.at[1], r.at[1])
        push(n_at(NEXT, o).at[:, 4096:], s, r, 3, x_dn)

    def gx_last(o):
        s, r = gxs.at[o], gxr.at[o]
        landed(n_at(FAR, o).at[:, :4096], s.at[2], r.at[2])
        landed(n_at(FAR, o).at[:, 4096:], s.at[3], r.at[3])

    order = (1, 7, 2, 6, 3, 5, 4)
    for o in order:
        push(nbuf.at[ti], gzs, gzr, o - 1, ten(x * NZ + (zl + o) % NZ))
    gx_start(0)
    before = 0
    for o in order:
        landed(n_at(OWN, o), gzs.at[o - 1], gzr.at[o - 1])
        gx_start(o)
        gx_next(before)
        before = o
    gx_next(before)
    outs = []

    def put(kx):
        rows = pl.ds(ring(x, kx) * NZ, NZ)
        copy = pltpu.make_async_copy(nbuf.at[rows], norm_hbm.at[rows], out_sem.at[kx])
        copy.start()
        outs.append(copy)

    put(OWN)
    put(PREV)
    put(NEXT)
    for o in (0, *order):
        gx_last(o)
    put(FAR)
    for copy in sent:
        copy.wait_send()
    for copy in outs:
        copy.wait()


def rope_tables(tok_count, ctx_len, head_dim):
    half = head_dim // 2
    inv_freq = np.float64(rope_theta) ** (-2.0 * np.arange(half) / head_dim)
    angles = (ctx_len - tok_count + np.arange(tok_count))[:, None] * inv_freq[None, :]
    cosine, sine = np.cos(angles), np.sin(angles)
    return (
        jnp.asarray(np.concatenate([cosine, cosine], axis=1), F32),
        jnp.asarray(np.concatenate([-sine, sine], axis=1), F32),
    )


def body(
    attn_input, residual, query_weight, query_bias, output_weight, cached_keys, cached_values,
    norm_gain,
):
    tok, width = attn_input.shape
    ctx_len, head_dim = cached_keys.shape[2:]
    own_count = tok // lax.axis_size("tensor")
    resid_rows = lax.dynamic_slice_in_dim(
        residual, lax.axis_index("tensor") * own_count, own_count, 0
    )
    cosine, sine = rope_tables(tok, ctx_len, head_dim)
    dma, vmem = pltpu.SemaphoreType.DMA, pltpu.VMEM
    any_spec = pl.BlockSpec(memory_space=pl.ANY)
    vmem_spec = pl.BlockSpec(memory_space=pltpu.VMEM)
    hidden, normed = pl.pallas_call(
        block_kernel,
        name="block",
        out_shape=(
            jax.ShapeDtypeStruct((own_count, width), BF16),
            jax.ShapeDtypeStruct((32, own_count, width), BF16),
        ),
        in_specs=[any_spec] * 5 + [vmem_spec] * 5,
        out_specs=(vmem_spec, any_spec),
        scratch_shapes=[
            vmem((2, 32, 2, 128, 256), BF16),
            vmem((tok, width), BF16),
            vmem((ctx_len, head_dim), BF16),
            vmem((ctx_len, head_dim), BF16),
            vmem((tok, 256), F32),
            vmem((tok, 256), BF16),
            vmem((4, 32, own_count, 2048), BF16),
            vmem((4, 2, 4, own_count, 2048), BF16),
            vmem((4, 2, 2, 4, own_count, 2048), BF16),
            vmem((4, 8, own_count, 2048), BF16),
            vmem((4, 7, own_count, 2048), BF16),
            vmem((own_count, width), F32),
            vmem((32, own_count, width), BF16),
            dma((5,)), dma((4,)),
            dma((2, 6)), dma((2, 6)),
            dma((2, 4, 6)), dma((2, 4, 6)),
            dma((2, 4, 4)), dma((2, 4, 4)),
            dma((4, 2)), dma((4, 2)),
            dma((4, 4)), dma((4, 4)),
            dma((4, 7)), dma((4, 7)),
            dma((7,)), dma((7,)),
            dma((8, 4)), dma((8, 4)),
        ],
        compiler_params=pltpu.CompilerParams(
            collective_id=0, has_side_effects=True, vmem_limit_bytes=48 * 1024 * 1024
        ),
    )(
        attn_input,
        query_weight.reshape(2, 128, 256),
        output_weight.reshape(2, 128, 256),
        cached_keys[0, 0],
        cached_values[0, 0],
        query_bias.reshape(1, -1),
        cosine,
        sine,
        resid_rows,
        norm_gain.reshape(1, -1),
    )
    return hidden, normed.reshape(tok, width)


def solution(mesh):
    return jax.shard_map(
        body,
        mesh=mesh,
        in_specs=(
            P("dp", None),
            P("dp", None),
            P("dp", "tensor"),
            P("tensor"),
            P("tensor", "dp"),
            P("dp", "tensor", None, None),
            P("dp", "tensor", None, None),
            P(),
        ),
        out_specs=(P(("dp", "tensor"), None), P("dp", None)),
        check_vma=False,
    )
```

```python
import jax
import jax.numpy as jnp
import numpy as np
from jax import lax
from jax.experimental import pallas as pl
from jax.experimental.pallas import tpu as pltpu
from jax.sharding import PartitionSpec as P

rope_theta = 1000000.0
norm_eps = 1e-06

NY, NH, NC = 4, 4, 2
NX, NZ = 4, 8
OWN, PREV, NEXT, FAR = 0, 1, 2, 3
STEP = (0, 3, 1, 2)
GROUP = ((0, 0), (1, 0), (1, 2048), (2, 0))
F32, BF16 = jnp.float32, jnp.bfloat16


def block_kernel(
    x_hbm, wq_hbm, wo_hbm, k_hbm, v_hbm, rope_hbm, res_hbm, bias_ref, gain_ref,
    hid_hbm, norm_hbm,
    wq, wo, xv, kv, vv, rope, resv, q, mixed, part, x1, x2, xsum, zr1, zmid, zr2, zacc, tot,
    n0, n1, n2, stage, hid, gain,
    loc, out_sem, zqs, zqr, yqs, yqr, dqs, dqr, zos, zor, yos, yor, dos, dor,
    p1s, p1r, p2s, p2r, t1s, t1r, t2s, t2r, gzs, gzr, gxs, gxr,
):
    dp = lax.axis_index("dp")
    ti = lax.axis_index("tensor")
    y, h, c = dp // (NH * NC), (dp // NC) % NH, dp % NC
    x, zl = ti // NZ, ti % NZ
    zq, zi = zl // 4, zl % 4

    def piece(yy, hh, cc):
        return yy * (NH * NC) + hh * NC + cc

    def ring(base, slot):
        return (base + STEP[slot]) % 4

    def dev(d):
        return {"dp": d}

    def ten(xx, quad, place):
        return {"tensor": xx * NZ + quad * 4 + place}

    h_up, h_dn = dev(piece(y, ring(h, NEXT), c)), dev(piece(y, ring(h, PREV), c))
    y_up, y_dn = dev(piece(ring(y, NEXT), h, c)), dev(piece(ring(y, PREV), h, c))
    sib = dev(piece(y, h, 1 - c))
    x_up, x_dn = ten(ring(x, NEXT), zq, zi), ten(ring(x, PREV), zq, zi)
    nb = (n0, n1, n2)
    mates = [None] + [ten(x, zq, (zi + o) % 4) for o in range(1, 4)]
    across = ten(x, 1 - zq, zi)

    locals_ = [
        pltpu.make_async_copy(wq_hbm, wq.at[dp], loc.at[0]),
        pltpu.make_async_copy(wo_hbm.at[:, :, :128], wo.at[dp, 0], loc.at[1]),
        pltpu.make_async_copy(wo_hbm.at[:, :, 128:], wo.at[dp, 1], loc.at[2]),
        pltpu.make_async_copy(x_hbm, xv, loc.at[3]),
        pltpu.make_async_copy(k_hbm, kv, loc.at[4]),
        pltpu.make_async_copy(v_hbm, vv, loc.at[5]),
        pltpu.make_async_copy(rope_hbm, rope, loc.at[6]),
        pltpu.make_async_copy(
            res_hbm.at[pl.ds(pl.multiple_of(ti // 2 * 8, 8), 8)], resv, loc.at[7]
        ),
    ]
    for copy in locals_:
        copy.start()

    barrier = pltpu.get_barrier_semaphore()
    partners = [h_up, h_dn, y_up, y_dn, sib, x_up, x_dn, across, *mates[1:]]
    for partner in partners:
        pl.semaphore_signal(
            barrier, inc=1, device_id=partner, device_id_type=pl.DeviceIdType.MESH
        )
    q[...] = jnp.zeros_like(q)
    for copy in locals_[:3]:
        copy.wait()
    pl.semaphore_wait(barrier, len(partners))

    sent = []

    def remote(src, dst, send_sem, recv_sem, target):
        return pltpu.make_async_remote_copy(
            src_ref=src, dst_ref=dst, send_sem=send_sem, recv_sem=recv_sem,
            device_id=target, device_id_type=pl.DeviceIdType.MESH,
        )

    def send(src, dst, send_sem, recv_sem, target):
        copy = remote(src, dst, send_sem, recv_sem, target)
        copy.start()
        sent.append(copy)
        return copy

    def left(*copies):
        for copy in copies:
            copy.wait_send()
            sent[:] = [other for other in sent if other is not copy]

    def landed(dst, send_sem, recv_sem):
        remote(dst, dst, send_sem, recv_sem, sib).wait_recv()

    def push(ref, s, r, i, target):
        return send(ref, ref, s.at[i], r.at[i], target)

    def q_at(ky, kh, half):
        return wq.at[piece(ring(y, ky), ring(h, kh), c), half]

    def q_start():
        return push(q_at(OWN, OWN, 0), zqs, zqr, 0, h_up), push(
            q_at(OWN, OWN, 1), zqs, zqr, 3, h_dn
        )

    def q_start_rest():
        push(q_at(OWN, OWN, 1), zqs, zqr, 1, h_up)
        push(q_at(OWN, OWN, 0), zqs, zqr, 4, h_dn)

    def qy_start(k, half):
        s, r = yqs.at[k], yqr.at[k]
        if half == 0:
            push(q_at(OWN, k, 0), s, r, 0, y_up)
            push(q_at(OWN, k, 0), s, r, 4, y_dn)
        else:
            push(q_at(OWN, k, 1), s, r, 3, y_dn)
            push(q_at(OWN, k, 1), s, r, 1, y_up)

    def qd_start(k, ky):
        push(wq.at[piece(ring(y, ky), ring(h, k), c)], dqs.at[k], dqr.at[k], ky, sib)

    def q_first():
        landed(q_at(OWN, PREV, 0), zqs.at[0], zqr.at[0])
        push(q_at(OWN, PREV, 0), zqs, zqr, 2, h_up)
        landed(q_at(OWN, NEXT, 1), zqs.at[3], zqr.at[3])
        push(q_at(OWN, NEXT, 1), zqs, zqr, 5, h_dn)
        qy_start(PREV, 0)
        qy_start(NEXT, 1)

    def q_second():
        landed(q_at(OWN, PREV, 1), zqs.at[1], zqr.at[1])
        qy_start(PREV, 1)
        qd_start(PREV, OWN)
        landed(q_at(OWN, NEXT, 0), zqs.at[4], zqr.at[4])
        qy_start(NEXT, 0)
        qd_start(NEXT, OWN)

    def q_third():
        landed(q_at(OWN, FAR, 0), zqs.at[2], zqr.at[2])
        qy_start(FAR, 0)
        landed(q_at(OWN, FAR, 1), zqs.at[5], zqr.at[5])
        qy_start(FAR, 1)
        qd_start(FAR, OWN)

    def qy_up(k):
        landed(q_at(PREV, k, 0), yqs.at[k, 0], yqr.at[k, 0])
        push(q_at(PREV, k, 0), yqs.at[k], yqr.at[k], 2, y_up)

    def qy_dn(k):
        landed(q_at(NEXT, k, 1), yqs.at[k, 3], yqr.at[k, 3])
        push(q_at(NEXT, k, 1), yqs.at[k], yqr.at[k], 5, y_dn)

    def qy_second(k):
        s, r = yqs.at[k], yqr.at[k]
        landed(q_at(PREV, k, 1), s.at[1], r.at[1])
        qd_start(k, PREV)
        landed(q_at(NEXT, k, 0), s.at[4], r.at[4])
        qd_start(k, NEXT)

    def qy_third(k):
        s, r = yqs.at[k], yqr.at[k]
        landed(q_at(FAR, k, 0), s.at[2], r.at[2])
        landed(q_at(FAR, k, 1), s.at[5], r.at[5])
        qd_start(k, FAR)

    def o_at(ky, kh, a):
        return wo.at[piece(ring(y, ky), ring(h, kh), c), a]

    def o_start(a):
        push(o_at(OWN, OWN, a), zos, zor, 2 * a, h_up)
        push(o_at(OWN, OWN, a), zos, zor, 2 * a + 1, h_dn)

    def oy_start(k, a):
        push(o_at(OWN, k, a), yos.at[k, a], yor.at[k, a], 0, y_up)
        push(o_at(OWN, k, a), yos.at[k, a], yor.at[k, a], 1, y_dn)

    def od_start(k, a, ky):
        push(o_at(ky, k, a), dos.at[k, a], dor.at[k, a], ky, sib)

    def o_first(a):
        landed(o_at(OWN, PREV, a), zos.at[2 * a], zor.at[2 * a])
        push(o_at(OWN, PREV, a).at[0], zos, zor, 4 + 2 * a, h_up)
        landed(o_at(OWN, NEXT, a), zos.at[2 * a + 1], zor.at[2 * a + 1])
        push(o_at(OWN, NEXT, a).at[1], zos, zor, 5 + 2 * a, h_dn)
        for k in (PREV, NEXT):
            oy_start(k, a)
            od_start(k, a, OWN)

    def o_third(a):
        landed(o_at(OWN, FAR, a).at[0], zos.at[4 + 2 * a], zor.at[4 + 2 * a])
        landed(o_at(OWN, FAR, a).at[1], zos.at[5 + 2 * a], zor.at[5 + 2 * a])
        oy_start(FAR, a)
        od_start(FAR, a, OWN)

    def oy_first(k, a):
        s, r = yos.at[k, a], yor.at[k, a]
        landed(o_at(PREV, k, a), s.at[0], r.at[0])
        push(o_at(PREV, k, a).at[0], s, r, 2, y_up)
        od_start(k, a, PREV)
        landed(o_at(NEXT, k, a), s.at[1], r.at[1])
        push(o_at(NEXT, k, a).at[1], s, r, 3, y_dn)
        od_start(k, a, NEXT)

    def oy_third(k, a):
        s, r = yos.at[k, a], yor.at[k, a]
        landed(o_at(FAR, k, a).at[0], s.at[2], r.at[2])
        landed(o_at(FAR, k, a).at[1], s.at[3], r.at[3])
        od_start(k, a, FAR)

    def project(k):
        hk = ring(h, k)
        for ky in range(4):
            ref = wq.at[piece(ring(y, ky), hk, 1 - c)]
            landed(ref, dqs.at[k, ky], dqr.at[k, ky])

        acc = q[...]
        for j in range(NY * NC):
            d = piece(j // NC, hk, j % NC)
            cols = xv[:, pl.ds(pl.multiple_of(d * 256, 256), 256)]
            acc = acc + jnp.dot(cols, wq[d].reshape(256, 256), preferred_element_type=F32)
        q[...] = acc

    def attend(head):
        cols = slice(head * 128, head * 128 + 128)
        proj = q[:, cols] + bias_ref[cols].astype(F32).reshape(1, 128)
        turned = proj * rope[0] + pltpu.roll(proj, 64, 1) * rope[1]
        scores = lax.dot_general(
            turned.astype(BF16), kv[...], (((1,), (1,)), ((), ())), preferred_element_type=F32
        ) * (1.0 / 128**0.5)
        rows = lax.broadcasted_iota(jnp.int32, scores.shape, 0)
        keys = lax.broadcasted_iota(jnp.int32, scores.shape, 1)
        scores = jnp.where(keys <= rows + (scores.shape[1] - scores.shape[0]), scores, -1e30)
        expo = jnp.exp(scores - jnp.max(scores, axis=-1, keepdims=True))
        soft = (expo / jnp.sum(expo, axis=-1, keepdims=True)).astype(BF16)
        mixed[:, cols] = jnp.dot(soft, vv[...], preferred_element_type=F32).astype(BF16)

    def partials(k, a):
        hk = ring(h, k)
        for ky in range(4):
            ref = wo.at[piece(ring(y, ky), hk, 1 - c), a]
            landed(ref, dos.at[k, a, ky], dor.at[k, a, ky])

        for j in range(NY * NC):
            d = piece(j // NC, hk, j % NC)
            out = jnp.dot(mixed[...], wo[d, a].reshape(256, 128), preferred_element_type=F32)
            part[k, a, :, :, j * 128 : j * 128 + 128] = out.astype(BF16).reshape(32, 4, 128)

    def rows_of(k, a, slot, at):
        return part.at[k, a, pl.ds(ring(x, slot) * NZ + at, 4)]

    def sum_first(k, a):
        s, r = p1s.at[k, a], p1r.at[k, a]
        send(rows_of(k, a, FAR, 0), x1.at[k, a, 0], s.at[0], r.at[0], x_up)
        send(rows_of(k, a, FAR, 4), x1.at[k, a, 1], s.at[1], r.at[1], x_dn)
        s, r = p2s.at[k, a], p2r.at[k, a]
        send(rows_of(k, a, NEXT, 4), x2.at[k, a, 0, 1], s.at[0], r.at[0], x_up)
        send(rows_of(k, a, PREV, 0), x2.at[k, a, 1, 0], s.at[1], r.at[1], x_dn)

    def sum_second(k, a):
        s, r = p2s.at[k, a], p2r.at[k, a]
        landed(x1.at[k, a, 0], p1s.at[k, a, 0], p1r.at[k, a, 0])
        own = rows_of(k, a, NEXT, 0)
        own[...] = (own[...].astype(F32) + x1[k, a, 0].astype(F32)).astype(BF16)
        send(own, x2.at[k, a, 0, 0], s.at[2], r.at[2], x_up)
        landed(x1.at[k, a, 1], p1s.at[k, a, 1], p1r.at[k, a, 1])
        own = rows_of(k, a, PREV, 4)
        own[...] = (own[...].astype(F32) + x1[k, a, 1].astype(F32)).astype(BF16)
        send(own, x2.at[k, a, 1, 1], s.at[3], r.at[3], x_dn)

    def sum_third(k, a):
        s, r = p2s.at[k, a], p2r.at[k, a]
        landed(x2.at[k, a, 0, 1], s.at[0], r.at[0])
        landed(x2.at[k, a, 1, 0], s.at[1], r.at[1])
        landed(x2.at[k, a, 0, 0], s.at[2], r.at[2])
        landed(x2.at[k, a, 1, 1], s.at[3], r.at[3])
        for half in range(2):
            own = rows_of(k, a, OWN, half * 4)[...].astype(F32)
            both = x2[k, a, 0, half].astype(F32) + x2[k, a, 1, half].astype(F32)
            xsum[k, a, half] = (own + both).astype(BF16)
        s, r = t1s.at[k, a], t1r.at[k, a]
        for o in range(1, 4):
            send(xsum.at[k, a, :, (zi + o) % 4], zr1.at[k, a, o - 1], s.at[o - 1], r.at[o - 1],
                 mates[o])

    def sum_fourth(k, a):
        for o in range(3):
            landed(zr1.at[k, a, o], t1s.at[k, a, o], t1r.at[k, a, o])

        def quad_sum(quad):
            acc = xsum[k, a, quad, zi].astype(F32)
            for o in range(3):
                acc = acc + zr1[k, a, o, quad].astype(F32)
            return acc

        zmid[k, a] = quad_sum(1 - zq).astype(BF16)
        send(zmid.at[k, a], zr2.at[k, a], t2s.at[k, a], t2r.at[k, a], across)
        zacc[k, a] = quad_sum(zq)

    def gathered(k, a):
        landed(zr2.at[k, a], t2s.at[k, a], t2r.at[k, a])
        acc = zacc[k, a] + zr2[k, a].astype(F32)
        hk = ring(h, k)
        g, base = GROUP[k]
        for j in range(NY * NC):
            d = piece(j // NC, hk, j % NC)
            at = pl.ds(pl.multiple_of(d * 256 + a * 128, 128), 128)
            total = tot[:, at] + acc[:, j * 128 : j * 128 + 128]
            tot[:, at] = total
            to = base + a * 1024 + j * 128
            nb[g][ti, :, to : to + 128] = total.astype(BF16)

    def n_at(g, kx, other, o):
        quad = (zq + other) % 2
        return nb[g].at[ring(x, kx) * NZ + quad * 4 + (zi + 4 - o) % 4]

    def gx_start(g, other, o):
        s, r = gxs.at[g, other, o], gxr.at[g, other, o]
        push(n_at(g, OWN, other, o), s, r, 0, x_up)
        push(n_at(g, OWN, other, o), s, r, 1, x_dn)

    def gx_next(g, other, o):
        s, r = gxs.at[g, other, o], gxr.at[g, other, o]
        half = nb[g].shape[-1] // 2
        landed(n_at(g, PREV, other, o), s.at[0], r.at[0])
        push(n_at(g, PREV, other, o).at[:, :half], s, r, 2, x_up)
        landed(n_at(g, NEXT, other, o), s.at[1], r.at[1])
        push(n_at(g, NEXT, other, o).at[:, half:], s, r, 3, x_dn)

    def gx_last(g, other, o):
        s, r = gxs.at[g, other, o], gxr.at[g, other, o]
        half = nb[g].shape[-1] // 2
        landed(n_at(g, FAR, other, o).at[:, :half], s.at[2], r.at[2])
        landed(n_at(g, FAR, other, o).at[:, half:], s.at[3], r.at[3])

    def gz_landed(g, other, o):
        landed(n_at(g, OWN, other, o), gzs.at[g, other, o], gzr.at[g, other, o])
        gx_start(g, other, o)

    def g_start(g):
        mine = n_at(g, OWN, 0, 0)
        send(mine, mine, gzs.at[g, 1, 0], gzr.at[g, 1, 0], across)
        for o in (1, 3, 2):
            push(mine, gzs.at[g, 0], gzr.at[g, 0], o, mates[o])
        gx_start(g, 0, 0)

    def g_across(g):
        gz_landed(g, 1, 0)
        for o in (1, 3, 2):
            push(n_at(g, OWN, 1, 0), gzs.at[g, 1], gzr.at[g, 1], o, mates[o])

    def g_quad(g, other):
        for o in (1, 3, 2):
            gz_landed(g, other, o)

    def g_ring(g, other):
        for o in (0, 1, 3, 2):
            gx_next(g, other, o)

    def put(kx):
        slot = ring(x, kx)
        rows8 = pl.ds(slot * NZ, NZ)
        hi, lo = nb[2][rows8, :, 2048:2176], nb[2][rows8, :, 2176:2304]
        scale = (hi.astype(F32) + lo.astype(F32)).reshape(32, 128)
        rows32 = pl.ds(pl.multiple_of(slot * 32, 32), 32)
        for k in range(4):
            hk = ring(h, k)
            g, base = GROUP[k]

            def one(i, carry, g=g, base=base, hk=hk):
                a, j = i // 8, i % 8
                d = piece(j // NC, hk, j % NC)
                at = pl.ds(pl.multiple_of(d * 256 + a * 128, 128), 128)
                src = pl.ds(pl.multiple_of(base + i * 128, 128), 128)
                vals = nb[g][rows8, :, src].astype(F32).reshape(32, 128)
                stage[rows32, at] = (vals * scale * gain[:, at]).astype(BF16)
                return carry

            lax.fori_loop(0, 16, one, 0, unroll=4)
        copy = pltpu.make_async_copy(stage.at[rows32], norm_hbm.at[rows32], out_sem.at[kx])
        copy.start()
        outs.append(copy)

    first = q_start()
    qy_start(OWN, 0)
    qy_start(OWN, 1)
    qd_start(OWN, OWN)
    qy_up(OWN)
    qy_dn(OWN)
    for a in range(2):
        oy_start(OWN, a)
        od_start(OWN, a, OWN)
    qy_second(OWN)
    qy_third(OWN)
    left(*first)
    q_start_rest()
    oy_first(OWN, 0)
    oy_first(OWN, 1)
    locals_[3].wait()
    project(OWN)
    locals_[7].wait()
    resid = resv[...].astype(F32)
    tot[...] = jnp.where(ti % 2 == 0, resid[:4], resid[4:])
    gain[...] = gain_ref[...].astype(F32).reshape(1, -1)
    oy_third(OWN, 0)
    oy_third(OWN, 1)
    q_first()
    qy_up(PREV)
    qy_dn(NEXT)
    q_second()
    o_start(0)
    qy_dn(PREV)
    qy_up(NEXT)
    for k in (PREV, NEXT):
        qy_second(k)
    for k in (PREV, NEXT):
        qy_third(k)
    project(PREV)
    project(NEXT)
    q_third()
    o_start(1)
    qy_up(FAR)
    qy_dn(FAR)
    qy_second(FAR)
    qy_third(FAR)
    project(FAR)
    locals_[4].wait()
    locals_[5].wait()
    locals_[6].wait()
    attend(0)
    attend(1)
    for a in range(2):
        partials(OWN, a)
        sum_first(OWN, a)
    o_first(0)
    for a in range(2):
        sum_second(OWN, a)
    for k in (PREV, NEXT):
        oy_first(k, 0)
    o_first(1)
    for a in range(2):
        sum_third(OWN, a)
    for k in (PREV, NEXT):
        oy_third(k, 0)
    for k in (PREV, NEXT):
        partials(k, 0)
        sum_first(k, 0)
    o_third(0)
    for k in (PREV, NEXT):
        oy_first(k, 1)
    for k in (PREV, NEXT):
        sum_second(k, 0)
    oy_first(FAR, 0)
    for k in (PREV, NEXT):
        oy_third(k, 1)
        partials(k, 1)
        sum_first(k, 1)
    for k in (PREV, NEXT):
        sum_third(k, 0)
    oy_third(FAR, 0)
    partials(FAR, 0)
    sum_first(FAR, 0)
    o_third(1)
    for k in (PREV, NEXT):
        sum_second(k, 1)
    for a in range(2):
        sum_fourth(OWN, a)
    for k in (PREV, NEXT):
        sum_third(k, 1)
    oy_first(FAR, 1)
    sum_second(FAR, 0)
    oy_third(FAR, 1)
    partials(FAR, 1)
    sum_first(FAR, 1)
    sum_third(FAR, 0)
    for a in range(2):
        gathered(OWN, a)
    g_start(0)
    for k in (PREV, NEXT):
        sum_fourth(k, 0)
    sum_second(FAR, 1)
    for k in (PREV, NEXT):
        sum_fourth(k, 1)
    sum_third(FAR, 1)
    sum_fourth(FAR, 0)
    g_quad(0, 0)
    g_across(0)
    for k in (PREV, NEXT):
        for a in range(2):
            gathered(k, a)
    g_start(1)
    sum_fourth(FAR, 1)
    gathered(FAR, 0)
    gathered(FAR, 1)
    total = tot[...]
    mean_square = jnp.mean(total * total, axis=-1, keepdims=True)
    scale = jnp.broadcast_to(lax.rsqrt(mean_square + norm_eps), (4, 128))
    high = scale.astype(BF16)
    nb[2][ti, :, 2048:2176] = high
    nb[2][ti, :, 2176:2304] = (scale - high.astype(F32)).astype(BF16)
    g_start(2)
    hid[...] = total.astype(BF16)
    outs = [pltpu.make_async_copy(hid, hid_hbm, out_sem.at[4])]
    outs[0].start()
    g_quad(1, 0)
    g_across(1)
    g_ring(0, 0)
    g_quad(0, 1)
    g_quad(2, 0)
    g_across(2)
    g_ring(1, 0)
    g_ring(0, 1)
    g_quad(1, 1)
    g_ring(2, 0)
    g_quad(2, 1)
    g_ring(1, 1)
    g_ring(2, 1)
    put(OWN)
    put(PREV)
    put(NEXT)
    for g in range(3):
        for other in range(2):
            for o in (0, 1, 3, 2):
                gx_last(g, other, o)
    put(FAR)
    for copy in sent:
        copy.wait_send()
    for copy in outs:
        copy.wait()


def rope_tables(tok_count, ctx_len, head_dim):
    half = head_dim // 2
    inv_freq = np.float64(rope_theta) ** (-2.0 * np.arange(half) / head_dim)
    angles = (ctx_len - tok_count + np.arange(tok_count))[:, None] * inv_freq[None, :]
    cosine, sine = np.cos(angles), np.sin(angles)
    cosine, sine = np.concatenate([cosine, cosine], 1), np.concatenate([-sine, sine], 1)
    return jnp.asarray(np.stack([cosine, sine]), F32)


def body(
    attn_input, residual, query_weight, query_bias, output_weight, cached_keys, cached_values,
    norm_gain,
):
    tok, width = attn_input.shape
    ctx_len, head_dim = cached_keys.shape[2:]
    own_count = tok // lax.axis_size("tensor")
    dma, vmem = pltpu.SemaphoreType.DMA, pltpu.VMEM
    any_spec = pl.BlockSpec(memory_space=pl.ANY)
    vmem_spec = pl.BlockSpec(memory_space=pltpu.VMEM)
    twice = lambda *shape: [dma(shape), dma(shape)]
    return pl.pallas_call(
        block_kernel,
        name="block",
        out_shape=(
            jax.ShapeDtypeStruct((own_count, width), BF16),
            jax.ShapeDtypeStruct((tok, width), BF16),
        ),
        in_specs=[any_spec] * 7 + [vmem_spec] * 2,
        out_specs=(any_spec, any_spec),
        scratch_shapes=[
            vmem((32, 2, 128, 256), BF16),
            vmem((32, 2, 2, 128, 128), BF16),
            vmem((tok, width), BF16),
            vmem((ctx_len, head_dim), BF16),
            vmem((ctx_len, head_dim), BF16),
            vmem((2, tok, head_dim), F32),
            vmem((8, width), BF16),
            vmem((tok, 256), F32),
            vmem((tok, 256), BF16),
            vmem((4, 2, 32, own_count, 1024), BF16),
            vmem((4, 2, 2, 4, own_count, 1024), BF16),
            vmem((4, 2, 2, 2, 4, own_count, 1024), BF16),
            vmem((4, 2, 2, 4, own_count, 1024), BF16),
            vmem((4, 2, 3, 2, own_count, 1024), BF16),
            vmem((4, 2, own_count, 1024), BF16),
            vmem((4, 2, own_count, 1024), BF16),
            vmem((4, 2, own_count, 1024), F32),
            vmem((own_count, width), F32),
            vmem((32, own_count, 2048), BF16),
            vmem((32, own_count, 4096), BF16),
            vmem((32, own_count, 2304), BF16),
            vmem((tok, width), BF16),
            vmem((own_count, width), BF16),
            vmem((1, width), F32),
            dma((8,)), dma((5,)),
            *twice(6), *twice(4, 6), *twice(4, 4),
            *twice(8), *twice(4, 2, 4), *twice(4, 2, 4),
            *twice(4, 2, 2), *twice(4, 2, 4), *twice(4, 2, 3), *twice(4, 2),
            *twice(3, 2, 4), *twice(3, 2, 4, 4),
        ],
        compiler_params=pltpu.CompilerParams(
            collective_id=0, has_side_effects=True, vmem_limit_bytes=67043328
        ),
    )(
        attn_input,
        query_weight.reshape(2, 128, 256),
        output_weight.reshape(2, 128, 256),
        cached_keys[0, 0],
        cached_values[0, 0],
        rope_tables(tok, ctx_len, head_dim),
        residual,
        query_bias,
        norm_gain,
    )


def solution(mesh):
    return jax.shard_map(
        body,
        mesh=mesh,
        in_specs=(
            P("dp", None),
            P("dp", None),
            P("dp", "tensor"),
            P("tensor"),
            P("tensor", "dp"),
            P("dp", "tensor", None, None),
            P("dp", "tensor", None, None),
            P(),
        ),
        out_specs=(P(("dp", "tensor"), None), P("dp", None)),
        check_vma=False,
    )
```

```python
import jax
import jax.numpy as jnp
import numpy as np
from jax import lax
from jax.experimental import pallas as pl
from jax.experimental.pallas import tpu as pltpu
from jax.sharding import PartitionSpec as P

rope_theta = 1000000.0
norm_eps = 1e-06

NY, NH, NC = 4, 4, 2
NX, NZ = 4, 8
OWN, PREV, NEXT, FAR = 0, 1, 2, 3
STEP = (0, 3, 1, 2)
INSIDE = tuple((other, o) for other in range(2) for o in range(4))
GROUP = ((0, 0), (1, 0), (1, 2048), (2, 0))
F32, BF16 = jnp.float32, jnp.bfloat16


class Shared:
    def __init__(self, index, own=None):
        self.index, self.own, self.at = index, own or {}, self

    def __getitem__(self, i):
        return Shared(self.own[i]) if i in self.own else self


def block_kernel(
    x_hbm, wq_hbm, wo_hbm, k_hbm, v_hbm, rope_hbm, res_hbm, bias_ref, gain_ref,
    hid_hbm, norm_hbm,
    wq, wo, xv, kv, vv, rope, resv, q, mixed, part, x1, x2, xsum, zr1, zmid, zr2, zacc, tot,
    n0, n1, n2, stage, hid, gain,
    loc, out_sem, left_sem, zqr, yqr, dqr, zor, yor, dor, p1r, p2r, t1r, t2r, gzr, gxr,
):
    dp = lax.axis_index("dp")
    ti = lax.axis_index("tensor")
    y, h, c = dp // (NH * NC), (dp // NC) % NH, dp % NC
    x, zl = ti // NZ, ti % NZ
    zq, zi = zl // 4, zl % 4

    def piece(yy, hh, cc):
        return yy * (NH * NC) + hh * NC + cc

    def ring(base, slot):
        return (base + STEP[slot]) % 4

    def dev(d):
        return {"dp": d}

    def ten(xx, quad, place):
        return {"tensor": xx * NZ + quad * 4 + place}

    h_up, h_dn = dev(piece(y, ring(h, NEXT), c)), dev(piece(y, ring(h, PREV), c))
    y_up, y_dn = dev(piece(ring(y, NEXT), h, c)), dev(piece(ring(y, PREV), h, c))
    sib = dev(piece(y, h, 1 - c))
    x_up, x_dn = ten(ring(x, NEXT), zq, zi), ten(ring(x, PREV), zq, zi)
    nb = (n0, n1, n2)
    mates = [None] + [ten(x, zq, (zi + o) % 4) for o in range(1, 4)]
    across = ten(x, 1 - zq, zi)

    locals_ = [
        pltpu.make_async_copy(wq_hbm, wq.at[dp], loc.at[0]),
        pltpu.make_async_copy(wo_hbm.at[:, :, :128], wo.at[dp, 0], loc.at[1]),
        pltpu.make_async_copy(wo_hbm.at[:, :, 128:], wo.at[dp, 1], loc.at[2]),
        pltpu.make_async_copy(x_hbm, xv, loc.at[3]),
        pltpu.make_async_copy(k_hbm, kv, loc.at[4]),
        pltpu.make_async_copy(v_hbm, vv, loc.at[5]),
        pltpu.make_async_copy(rope_hbm, rope, loc.at[6]),
        pltpu.make_async_copy(
            res_hbm.at[pl.ds(pl.multiple_of(ti // 2 * 8, 8), 8)], resv, loc.at[7]
        ),
    ]
    for copy in locals_:
        copy.start()

    barrier = pltpu.get_barrier_semaphore()
    partners = [h_up, h_dn, y_up, y_dn, sib, x_up, x_dn, across, *mates[1:]]
    for partner in partners:
        pl.semaphore_signal(
            barrier, inc=1, device_id=partner, device_id_type=pl.DeviceIdType.MESH
        )
    q[...] = jnp.zeros_like(q)
    for copy in locals_[:3]:
        copy.wait()
    pl.semaphore_wait(barrier, len(partners))

    zqs, yqs, dqs = Shared(0, {0: 1, 3: 2, 2: 3, 5: 4}), Shared(0), Shared(0)
    zos, yos, dos = Shared(5), Shared(5), Shared(5)
    p1s, p2s, t1s, t2s = Shared(6), Shared(6), Shared(7), Shared(8)
    gzs = gxs = Shared(9, {(g, *at): 9 + g for g in range(3) for at in INSIDE})

    def remote(src, dst, send_sem, recv_sem, target):
        return pltpu.make_async_remote_copy(
            src_ref=src, dst_ref=dst, send_sem=send_sem, recv_sem=recv_sem,
            device_id=target, device_id_type=pl.DeviceIdType.MESH,
        )

    def send(src, dst, send_sem, recv_sem, target):
        copy = remote(src, dst, left_sem.at[send_sem.index], recv_sem, target)
        copy.start()
        return copy

    def left(*copies):
        for copy in copies:
            copy.wait_send()

    def landed(dst, send_sem, recv_sem):
        remote(dst, dst, left_sem.at[send_sem.index], recv_sem, sib).wait_recv()

    def push(ref, s, r, i, target):
        return send(ref, ref, s.at[i], r.at[i], target)

    def q_at(ky, kh, half):
        return wq.at[piece(ring(y, ky), ring(h, kh), c), half]

    def q_start():
        return push(q_at(OWN, OWN, 0), zqs, zqr, 0, h_up), push(
            q_at(OWN, OWN, 1), zqs, zqr, 3, h_dn
        )

    def q_start_rest():
        push(q_at(OWN, OWN, 1), zqs, zqr, 1, h_up)
        push(q_at(OWN, OWN, 0), zqs, zqr, 4, h_dn)

    def qy_start(k, half):
        s, r = yqs.at[k], yqr.at[k]
        if half == 0:
            push(q_at(OWN, k, 0), s, r, 0, y_up)
            push(q_at(OWN, k, 0), s, r, 4, y_dn)
        else:
            push(q_at(OWN, k, 1), s, r, 3, y_dn)
            push(q_at(OWN, k, 1), s, r, 1, y_up)

    def qd_start(k, ky):
        push(wq.at[piece(ring(y, ky), ring(h, k), c)], dqs.at[k], dqr.at[k], ky, sib)

    def q_first():
        landed(q_at(OWN, PREV, 0), zqs.at[0], zqr.at[0])
        up = push(q_at(OWN, PREV, 0), zqs, zqr, 2, h_up)
        landed(q_at(OWN, NEXT, 1), zqs.at[3], zqr.at[3])
        dn = push(q_at(OWN, NEXT, 1), zqs, zqr, 5, h_dn)
        qy_start(PREV, 0)
        qy_start(NEXT, 1)
        return up, dn

    def q_second():
        landed(q_at(OWN, PREV, 1), zqs.at[1], zqr.at[1])
        qy_start(PREV, 1)
        qd_start(PREV, OWN)
        landed(q_at(OWN, NEXT, 0), zqs.at[4], zqr.at[4])
        qy_start(NEXT, 0)
        qd_start(NEXT, OWN)

    def q_third():
        landed(q_at(OWN, FAR, 0), zqs.at[2], zqr.at[2])
        qy_start(FAR, 0)
        landed(q_at(OWN, FAR, 1), zqs.at[5], zqr.at[5])
        qy_start(FAR, 1)
        qd_start(FAR, OWN)

    def qy_up(k):
        landed(q_at(PREV, k, 0), yqs.at[k, 0], yqr.at[k, 0])
        push(q_at(PREV, k, 0), yqs.at[k], yqr.at[k], 2, y_up)

    def qy_dn(k):
        landed(q_at(NEXT, k, 1), yqs.at[k, 3], yqr.at[k, 3])
        push(q_at(NEXT, k, 1), yqs.at[k], yqr.at[k], 5, y_dn)

    def qy_second(k):
        s, r = yqs.at[k], yqr.at[k]
        landed(q_at(PREV, k, 1), s.at[1], r.at[1])
        qd_start(k, PREV)
        landed(q_at(NEXT, k, 0), s.at[4], r.at[4])
        qd_start(k, NEXT)

    def qy_third(k):
        s, r = yqs.at[k], yqr.at[k]
        landed(q_at(FAR, k, 0), s.at[2], r.at[2])
        landed(q_at(FAR, k, 1), s.at[5], r.at[5])
        qd_start(k, FAR)

    def o_at(ky, kh, a):
        return wo.at[piece(ring(y, ky), ring(h, kh), c), a]

    def o_start(a):
        push(o_at(OWN, OWN, a), zos, zor, 2 * a, h_up)
        push(o_at(OWN, OWN, a), zos, zor, 2 * a + 1, h_dn)

    def oy_start(k, a):
        push(o_at(OWN, k, a), yos.at[k, a], yor.at[k, a], 0, y_up)
        push(o_at(OWN, k, a), yos.at[k, a], yor.at[k, a], 1, y_dn)

    def od_start(k, a, ky):
        push(o_at(ky, k, a), dos.at[k, a], dor.at[k, a], ky, sib)

    def o_first(a):
        landed(o_at(OWN, PREV, a), zos.at[2 * a], zor.at[2 * a])
        push(o_at(OWN, PREV, a).at[0], zos, zor, 4 + 2 * a, h_up)
        landed(o_at(OWN, NEXT, a), zos.at[2 * a + 1], zor.at[2 * a + 1])
        push(o_at(OWN, NEXT, a).at[1], zos, zor, 5 + 2 * a, h_dn)
        for k in (PREV, NEXT):
            oy_start(k, a)
            od_start(k, a, OWN)

    def o_third(a):
        landed(o_at(OWN, FAR, a).at[0], zos.at[4 + 2 * a], zor.at[4 + 2 * a])
        landed(o_at(OWN, FAR, a).at[1], zos.at[5 + 2 * a], zor.at[5 + 2 * a])
        oy_start(FAR, a)
        od_start(FAR, a, OWN)

    def oy_first(k, a):
        s, r = yos.at[k, a], yor.at[k, a]
        landed(o_at(PREV, k, a), s.at[0], r.at[0])
        push(o_at(PREV, k, a).at[0], s, r, 2, y_up)
        od_start(k, a, PREV)
        landed(o_at(NEXT, k, a), s.at[1], r.at[1])
        push(o_at(NEXT, k, a).at[1], s, r, 3, y_dn)
        od_start(k, a, NEXT)

    def oy_third(k, a):
        s, r = yos.at[k, a], yor.at[k, a]
        landed(o_at(FAR, k, a).at[0], s.at[2], r.at[2])
        landed(o_at(FAR, k, a).at[1], s.at[3], r.at[3])
        od_start(k, a, FAR)

    def project(k):
        hk = ring(h, k)
        for ky in range(4):
            ref = wq.at[piece(ring(y, ky), hk, 1 - c)]
            landed(ref, dqs.at[k, ky], dqr.at[k, ky])

        acc = q[...]
        for j in range(NY * NC):
            d = piece(j // NC, hk, j % NC)
            cols = xv[:, pl.ds(pl.multiple_of(d * 256, 256), 256)]
            acc = acc + jnp.dot(cols, wq[d].reshape(256, 256), preferred_element_type=F32)
        q[...] = acc

    def attend(head):
        cols = slice(head * 128, head * 128 + 128)
        proj = q[:, cols] + bias_ref[cols].astype(F32).reshape(1, 128)
        turned = proj * rope[0] + pltpu.roll(proj, 64, 1) * rope[1]
        scores = lax.dot_general(
            turned.astype(BF16), kv[...], (((1,), (1,)), ((), ())), preferred_element_type=F32
        ) * (1.0 / 128**0.5)
        rows = lax.broadcasted_iota(jnp.int32, scores.shape, 0)
        keys = lax.broadcasted_iota(jnp.int32, scores.shape, 1)
        scores = jnp.where(keys <= rows + (scores.shape[1] - scores.shape[0]), scores, -1e30)
        expo = jnp.exp(scores - jnp.max(scores, axis=-1, keepdims=True))
        soft = (expo / jnp.sum(expo, axis=-1, keepdims=True)).astype(BF16)
        mixed[:, cols] = jnp.dot(soft, vv[...], preferred_element_type=F32).astype(BF16)

    def partials(k, a):
        hk = ring(h, k)
        for ky in range(4):
            ref = wo.at[piece(ring(y, ky), hk, 1 - c), a]
            landed(ref, dos.at[k, a, ky], dor.at[k, a, ky])

        for j in range(NY * NC):
            d = piece(j // NC, hk, j % NC)
            out = jnp.dot(mixed[...], wo[d, a].reshape(256, 128), preferred_element_type=F32)
            part[k, a, :, :, j * 128 : j * 128 + 128] = out.astype(BF16).reshape(32, 4, 128)

    def rows_of(k, a, slot, at):
        return part.at[k, a, pl.ds(ring(x, slot) * NZ + at, 4)]

    def sum_first(k, a):
        s, r = p1s.at[k, a], p1r.at[k, a]
        send(rows_of(k, a, FAR, 0), x1.at[k, a, 0], s.at[0], r.at[0], x_up)
        send(rows_of(k, a, FAR, 4), x1.at[k, a, 1], s.at[1], r.at[1], x_dn)
        s, r = p2s.at[k, a], p2r.at[k, a]
        send(rows_of(k, a, NEXT, 4), x2.at[k, a, 0, 1], s.at[0], r.at[0], x_up)
        send(rows_of(k, a, PREV, 0), x2.at[k, a, 1, 0], s.at[1], r.at[0], x_dn)

    def sum_second(k, a):
        s, r = p2s.at[k, a], p2r.at[k, a]
        landed(x1.at[k, a, 0], p1s.at[k, a, 0], p1r.at[k, a, 0])
        own = rows_of(k, a, NEXT, 0)
        own[...] = (own[...].astype(F32) + x1[k, a, 0].astype(F32)).astype(BF16)
        send(own, x2.at[k, a, 0, 0], s.at[2], r.at[0], x_up)
        landed(x1.at[k, a, 1], p1s.at[k, a, 1], p1r.at[k, a, 1])
        own = rows_of(k, a, PREV, 4)
        own[...] = (own[...].astype(F32) + x1[k, a, 1].astype(F32)).astype(BF16)
        send(own, x2.at[k, a, 1, 1], s.at[3], r.at[0], x_dn)

    def sum_third(k, a):
        s, r = p2s.at[k, a], p2r.at[k, a]
        landed(x2.at[k, a], s.at[0], r.at[0])
        for half in range(2):
            own = rows_of(k, a, OWN, half * 4)[...].astype(F32)
            both = x2[k, a, 0, half].astype(F32) + x2[k, a, 1, half].astype(F32)
            xsum[k, a, half] = (own + both).astype(BF16)
        s, r = t1s.at[k, a], t1r.at[k, a]
        for o in range(1, 4):
            send(xsum.at[k, a, :, (zi + o) % 4], zr1.at[k, a, o - 1], s.at[o - 1], r.at[0],
                 mates[o])

    def sum_fourth(k, a):
        landed(zr1.at[k, a], t1s.at[k, a], t1r.at[k, a, 0])

        def quad_sum(quad):
            acc = xsum[k, a, quad, zi].astype(F32)
            for o in range(3):
                acc = acc + zr1[k, a, o, quad].astype(F32)
            return acc

        zmid[k, a] = quad_sum(1 - zq).astype(BF16)
        send(zmid.at[k, a], zr2.at[k, a], t2s.at[k, a], t2r.at[k, a], across)
        zacc[k, a] = quad_sum(zq)

    def gathered(k, a):
        landed(zr2.at[k, a], t2s.at[k, a], t2r.at[k, a])
        acc = zacc[k, a] + zr2[k, a].astype(F32)
        hk = ring(h, k)
        g, base = GROUP[k]
        for j in range(NY * NC):
            d = piece(j // NC, hk, j % NC)
            at = pl.ds(pl.multiple_of(d * 256 + a * 128, 128), 128)
            total = tot[:, at] + acc[:, j * 128 : j * 128 + 128]
            tot[:, at] = total
            to = base + a * 1024 + j * 128
            nb[g][ti, :, to : to + 128] = total.astype(BF16)

    def n_at(g, kx, other, o):
        quad = (zq + other) % 2
        return nb[g].at[ring(x, kx) * NZ + quad * 4 + (zi + 4 - o) % 4]

    def gx_start(g, other, o):
        s, r = gxs.at[g, other, o], gxr.at[g, other, o]
        push(n_at(g, OWN, other, o), s, r, 0, x_up)
        push(n_at(g, OWN, other, o), s, r, 1, x_dn)

    def gx_next(g, other, o):
        s, r = gxs.at[g, other, o], gxr.at[g, other, o]
        half = nb[g].shape[-1] // 2
        landed(n_at(g, PREV, other, o), s.at[0], r.at[0])
        push(n_at(g, PREV, other, o).at[:, :half], s, r, 2, x_up)
        landed(n_at(g, NEXT, other, o), s.at[1], r.at[1])
        push(n_at(g, NEXT, other, o).at[:, half:], s, r, 2, x_dn)

    def gx_last(g, other, o):
        s, r = gxs.at[g, other, o], gxr.at[g, other, o]
        landed(n_at(g, FAR, other, o), s.at[2], r.at[2])

    def gz_landed(g, other, o):
        landed(n_at(g, OWN, other, o), gzs.at[g, other, o], gzr.at[g, other, o])
        gx_start(g, other, o)

    def g_start(g):
        mine = n_at(g, OWN, 0, 0)
        send(mine, mine, gzs.at[g, 1, 0], gzr.at[g, 1, 0], across)
        for o in (1, 3, 2):
            push(mine, gzs.at[g, 0, o], gzr.at[g, 0], o, mates[o])
        gx_start(g, 0, 0)

    def g_across(g):
        gz_landed(g, 1, 0)
        for o in (1, 3, 2):
            push(n_at(g, OWN, 1, 0), gzs.at[g, 1, o], gzr.at[g, 1], o, mates[o])

    def g_quad(g, other):
        for o in (1, 3, 2):
            gz_landed(g, other, o)

    def g_ring(g, other):
        for o in (0, 1, 3, 2):
            gx_next(g, other, o)

    def put(kx):
        slot = ring(x, kx)
        rows8 = pl.ds(slot * NZ, NZ)
        hi, lo = nb[2][rows8, :, 2048:2176], nb[2][rows8, :, 2176:2304]
        scale = (hi.astype(F32) + lo.astype(F32)).reshape(32, 128)
        rows32 = pl.ds(pl.multiple_of(slot * 32, 32), 32)
        for k in range(4):
            hk = ring(h, k)
            g, base = GROUP[k]

            def one(i, carry, g=g, base=base, hk=hk):
                a, j = i // 8, i % 8
                d = piece(j // NC, hk, j % NC)
                at = pl.ds(pl.multiple_of(d * 256 + a * 128, 128), 128)
                src = pl.ds(pl.multiple_of(base + i * 128, 128), 128)
                vals = nb[g][rows8, :, src].astype(F32).reshape(32, 128)
                stage[rows32, at] = (vals * scale * gain[:, at]).astype(BF16)
                return carry

            lax.fori_loop(0, 16, one, 0, unroll=4)
        copy = pltpu.make_async_copy(stage.at[rows32], norm_hbm.at[rows32], out_sem.at[kx])
        copy.start()
        outs.append(copy)

    first = q_start()
    qy_start(OWN, 0)
    qy_start(OWN, 1)
    qd_start(OWN, OWN)
    qy_up(OWN)
    qy_dn(OWN)
    for a in range(2):
        oy_start(OWN, a)
        od_start(OWN, a, OWN)
    qy_second(OWN)
    qy_third(OWN)
    left(*first)
    q_start_rest()
    oy_first(OWN, 0)
    oy_first(OWN, 1)
    locals_[3].wait()
    project(OWN)
    locals_[7].wait()
    resid = resv[...].astype(F32)
    tot[...] = jnp.where(ti % 2 == 0, resid[:4], resid[4:])
    gain[...] = gain_ref[...].astype(F32).reshape(1, -1)
    oy_third(OWN, 0)
    oy_third(OWN, 1)
    far = q_first()
    qy_up(PREV)
    qy_dn(NEXT)
    q_second()
    left(*far)
    o_start(0)
    qy_dn(PREV)
    qy_up(NEXT)
    for k in (PREV, NEXT):
        qy_second(k)
    for k in (PREV, NEXT):
        qy_third(k)
    project(PREV)
    project(NEXT)
    q_third()
    o_start(1)
    qy_up(FAR)
    qy_dn(FAR)
    qy_second(FAR)
    qy_third(FAR)
    project(FAR)
    locals_[4].wait()
    locals_[5].wait()
    locals_[6].wait()
    attend(0)
    attend(1)
    for a in range(2):
        partials(OWN, a)
        sum_first(OWN, a)
    o_first(0)
    for a in range(2):
        sum_second(OWN, a)
    for k in (PREV, NEXT):
        oy_first(k, 0)
    o_first(1)
    for a in range(2):
        sum_third(OWN, a)
    for k in (PREV, NEXT):
        oy_third(k, 0)
    for k in (PREV, NEXT):
        partials(k, 0)
        sum_first(k, 0)
    o_third(0)
    for k in (PREV, NEXT):
        oy_first(k, 1)
    for k in (PREV, NEXT):
        sum_second(k, 0)
    oy_first(FAR, 0)
    for k in (PREV, NEXT):
        oy_third(k, 1)
        partials(k, 1)
        sum_first(k, 1)
    for k in (PREV, NEXT):
        sum_third(k, 0)
    oy_third(FAR, 0)
    partials(FAR, 0)
    sum_first(FAR, 0)
    o_third(1)
    for k in (PREV, NEXT):
        sum_second(k, 1)
    for a in range(2):
        sum_fourth(OWN, a)
    for k in (PREV, NEXT):
        sum_third(k, 1)
    oy_first(FAR, 1)
    sum_second(FAR, 0)
    oy_third(FAR, 1)
    partials(FAR, 1)
    sum_first(FAR, 1)
    sum_third(FAR, 0)
    for a in range(2):
        gathered(OWN, a)
    g_start(0)
    for k in (PREV, NEXT):
        sum_fourth(k, 0)
    sum_second(FAR, 1)
    for k in (PREV, NEXT):
        sum_fourth(k, 1)
    sum_third(FAR, 1)
    sum_fourth(FAR, 0)
    g_quad(0, 0)
    g_across(0)
    for k in (PREV, NEXT):
        for a in range(2):
            gathered(k, a)
    g_start(1)
    sum_fourth(FAR, 1)
    gathered(FAR, 0)
    gathered(FAR, 1)
    total = tot[...]
    mean_square = jnp.mean(total * total, axis=-1, keepdims=True)
    scale = jnp.broadcast_to(lax.rsqrt(mean_square + norm_eps), (4, 128))
    high = scale.astype(BF16)
    nb[2][ti, :, 2048:2176] = high
    nb[2][ti, :, 2176:2304] = (scale - high.astype(F32)).astype(BF16)
    g_start(2)
    hid[...] = total.astype(BF16)
    outs = [pltpu.make_async_copy(hid, hid_hbm, out_sem.at[4])]
    outs[0].start()
    g_quad(1, 0)
    g_across(1)
    g_ring(0, 0)
    g_quad(0, 1)
    g_quad(2, 0)
    g_across(2)
    g_ring(1, 0)
    g_ring(0, 1)
    g_quad(1, 1)
    g_ring(2, 0)
    g_quad(2, 1)
    put(OWN)
    g_ring(1, 1)
    g_ring(2, 1)
    put(PREV)
    put(NEXT)
    for g in range(3):
        for other in range(2):
            for o in (0, 1, 3, 2):
                gx_last(g, other, o)
    put(FAR)
    all_sent = [
        (wq.at[:29], 0), (wo.at[:31], 5), (part.at[:3], 6), (zr1, 7), (zr2, 8),
        *((rows.at[:31], 9 + g) for g, rows in enumerate(nb)),
    ]
    for ref, i in all_sent:
        remote(ref, ref, left_sem.at[i], zqr.at[0], sib).wait_send()
    for copy in outs:
        copy.wait()


def rope_tables(tok_count, ctx_len, head_dim):
    half = head_dim // 2
    inv_freq = np.float64(rope_theta) ** (-2.0 * np.arange(half) / head_dim)
    angles = (ctx_len - tok_count + np.arange(tok_count))[:, None] * inv_freq[None, :]
    cosine, sine = np.cos(angles), np.sin(angles)
    cosine, sine = np.concatenate([cosine, cosine], 1), np.concatenate([-sine, sine], 1)
    return jnp.asarray(np.stack([cosine, sine]), F32)


def body(
    attn_input, residual, query_weight, query_bias, output_weight, cached_keys, cached_values,
    norm_gain,
):
    tok, width = attn_input.shape
    ctx_len, head_dim = cached_keys.shape[2:]
    own_count = tok // lax.axis_size("tensor")
    dma, vmem = pltpu.SemaphoreType.DMA, pltpu.VMEM
    any_spec = pl.BlockSpec(memory_space=pl.ANY)
    vmem_spec = pl.BlockSpec(memory_space=pltpu.VMEM)
    return pl.pallas_call(
        block_kernel,
        name="block",
        out_shape=(
            jax.ShapeDtypeStruct((own_count, width), BF16),
            jax.ShapeDtypeStruct((tok, width), BF16),
        ),
        in_specs=[any_spec] * 7 + [vmem_spec] * 2,
        out_specs=(any_spec, any_spec),
        scratch_shapes=[
            vmem((32, 2, 128, 256), BF16),
            vmem((32, 2, 2, 128, 128), BF16),
            vmem((tok, width), BF16),
            vmem((ctx_len, head_dim), BF16),
            vmem((ctx_len, head_dim), BF16),
            vmem((2, tok, head_dim), F32),
            vmem((8, width), BF16),
            vmem((tok, 256), F32),
            vmem((tok, 256), BF16),
            vmem((4, 2, 32, own_count, 1024), BF16),
            vmem((4, 2, 2, 4, own_count, 1024), BF16),
            vmem((4, 2, 2, 2, 4, own_count, 1024), BF16),
            vmem((4, 2, 2, 4, own_count, 1024), BF16),
            vmem((4, 2, 3, 2, own_count, 1024), BF16),
            vmem((4, 2, own_count, 1024), BF16),
            vmem((4, 2, own_count, 1024), BF16),
            vmem((4, 2, own_count, 1024), F32),
            vmem((own_count, width), F32),
            vmem((32, own_count, 2048), BF16),
            vmem((32, own_count, 4096), BF16),
            vmem((32, own_count, 2304), BF16),
            vmem((tok, width), BF16),
            vmem((own_count, width), BF16),
            vmem((1, width), F32),
            dma((8,)), dma((5,)),
            dma((12,)),
            dma((6,)), dma((4, 6)), dma((4, 4)),
            dma((8,)), dma((4, 2, 4)), dma((4, 2, 4)),
            dma((4, 2, 2)), dma((4, 2, 1)), dma((4, 2, 1)), dma((4, 2)),
            dma((3, 2, 4)), dma((3, 2, 4, 3)),
        ],
        compiler_params=pltpu.CompilerParams(
            collective_id=0, has_side_effects=True, vmem_limit_bytes=67043328
        ),
    )(
        attn_input,
        query_weight.reshape(2, 128, 256),
        output_weight.reshape(2, 128, 256),
        cached_keys[0, 0],
        cached_values[0, 0],
        rope_tables(tok, ctx_len, head_dim),
        residual,
        query_bias,
        norm_gain,
    )


def solution(mesh):
    return jax.shard_map(
        body,
        mesh=mesh,
        in_specs=(
            P("dp", None),
            P("dp", None),
            P("dp", "tensor"),
            P("tensor"),
            P("tensor", "dp"),
            P("dp", "tensor", None, None),
            P("dp", "tensor", None, None),
            P(),
        ),
        out_specs=(P(("dp", "tensor"), None), P("dp", None)),
        check_vma=False,
    )
```
